32 devices in a mesh: ctx: 8 (over y, x, core), head: 4 (over z).
Axes of the slice: x: 2, y: 2, z: 4, core: 2. Of those that a mesh axis runs over, the one named last changes fastest.
Arguments:
- prefix: bfloat16 [65536, 1024], P(('ctx', 'head')), may hold values from -6 to 6
- keep_blocks: int32 [4, 8, 16], P('head', 'ctx'), may hold values from 0 to 15, each once within a row
- keep_count: int32 [4, 8], P('head', 'ctx'), may hold values from 1 to 16, 64 in all within a row
- latent_inputs: bfloat16 [128, 1024], P('ctx'), may hold values from -6 to 6
- latent_pos: int32 [128], replicated, may hold values from 0 to 65535
- w_query: bfloat16 [1024, 1024], P(None, 'head')
- w_key: bfloat16 [1024, 1024], replicated, may hold values from -0.1875 to 0.1875
- w_value: bfloat16 [1024, 1024], replicated, may hold values from -0.1875 to 0.1875
Outputs:
- attended: bfloat16 [128, 1024], P('ctx', 'head')
The draws below stay inside these ranges and needn't reach their ends.
Inputs may be any that keep to these rules, and one draw needn't show every extreme that they name: keep_blocks[h, c, :] lists each of the 16 block numbers once; the first keep_count[h, c] entries are the kept blocks. For every index h, keep_count[h, :] sums to 64, and its largest entry is 16.
All inputs are finite; a program needn't handle non-finite values. No bound on the sum of `keep_count` on one device may be relied on, other than what follows from the above.
Results may differ from the reference program's by a relative error of at most 0.0085.
The reference program's roundings to bfloat16 on the way count: a program that leaves them out, or rounds other values in their place, can miss the bound.
Values may be sent and summed in bfloat16 or wider, within the bound.
No kernel may reach another device: no remote copies, remote signals or barrier semaphores. Data moves between devices by JAX's collectives and lax.ppermute only.
A program may use at most 128 MiB of HBM per device.

```python
import math
import jax
import jax.numpy as jnp
import numpy as np
from jax import lax

D = 1024
HEADS = 16
HD = 64
BLOCK = 128
BLK_DEV = 16
LAT_DEV = 16
ROWS = 65536
LAT = 128
N_CTX = 8
N_HEAD = 4


def draw_w_query(key, part):
    raw_weights = jax.random.normal(key, (D, HEADS * HD), jnp.float32) * D ** (-0.5)
    return raw_weights.astype(jnp.bfloat16)


def plant(result, rng, low, largest):
    dims = result.shape
    spot = [jax.random.randint(jax.random.fold_in(rng, axis), (), 0, dims[axis]) for axis in range(len(dims))]
    result = result.at[tuple(spot)].set(low)
    longest = dims.index(max(dims))
    spot[longest] = (spot[longest] + 1) % dims[longest]
    return result.at[tuple(spot)].set(largest)


def level_of(rng, extent, cuts, smallest, high):
    gain, own = 1.0, jax.random.fold_in(rng, 6)
    for position, parts in cuts:
        heights = jnp.exp(jax.random.uniform(jax.random.fold_in(own, position), (parts,), jnp.float32, smallest / len(cuts), high / len(cuts)))
        gain = gain * jnp.repeat(heights, extent[position] // parts).reshape([-1 if axis == position else 1 for axis in range(len(extent))])
    return gain


def length_profile(number_of, total, bound, skew):
    portions = [(1 << 20) // math.isqrt(grade ** skew) + 1 for grade in range(2, number_of + 1)]
    rest, counts = total - bound - (number_of - 1), [1] * (number_of - 1)
    while rest > 0:
        candidates = [i for i in range(number_of - 1) if counts[i] < bound]
        mass, budget = sum([portions[i] for i in candidates]), rest
        for i in candidates:
            more = min(bound - counts[i], max(1, budget * portions[i] // mass), rest)
            counts[i] = counts[i] + more
            rest = rest - more
    return np.array([bound] + counts)


def uneven(key, count, total, bound, lean):
    if count == 2:
        one = jax.random.randint(key, (), max(1, total - bound), min(bound, total - 1) + 1)
        return jnp.stack([one, total - one])
    sizes = jnp.asarray(length_profile(count, total, bound, lean), jnp.int32)
    pairs = (count - 1) // 2
    source_of, sink = sizes[1:1 + 2 * pairs:2], sizes[2:2 + 2 * pairs:2]
    slack = jnp.minimum(source_of - 1, bound - sink)
    moved = jax.random.randint(jax.random.fold_in(key, 1), (pairs,), 0, 1 << 20) % (slack + 1)
    sizes = sizes.at[1:1 + 2 * pairs:2].set(source_of - moved).at[2:2 + 2 * pairs:2].set(sink + moved)
    return sizes[jax.random.permutation(jax.random.fold_in(key, 2), count)]


def bell_draw(own_key, shape, width, bound, pieces=(), kind=jnp.bfloat16):
    values = jax.random.normal(own_key, shape, jnp.float32) * width
    if len(pieces) > 0:
        values = level_of(own_key, shape, pieces, -0.22, 0.18) * values
    return jnp.clip(values, min=-bound, max=bound).astype(kind)


def setup_inputs(seed: int = 0) -> dict:
    key_list = jax.random.split(jax.random.key(seed), 9)
    return {
        "prefix": bell_draw(key_list[0], (ROWS, D), 1.0, 6.0, ((0, 32),)),
        "keep_blocks": jax.vmap(lambda own: jax.random.permutation(own, BLK_DEV))(jax.random.split(key_list[1], N_HEAD * N_CTX)).reshape((N_HEAD, N_CTX, BLK_DEV)).astype(jnp.int32),
        "keep_count": jax.vmap(lambda own: uneven(own, N_CTX, N_CTX * (BLK_DEV // 2), BLK_DEV, 2))(jax.random.split(key_list[2], N_HEAD)).reshape((N_HEAD, N_CTX)).astype(jnp.int32),
        "latent_inputs": bell_draw(key_list[3], (LAT, D), 1.0, 6.0, ((0, 8),)),
        "latent_pos": plant(jax.random.randint(key_list[4], (LAT,), 0, ROWS), jax.random.fold_in(key_list[4], 1), 0, ROWS - 1).astype(jnp.int32),
        "w_query": draw_w_query(jax.random.fold_in(key_list[8], 71), 0),
        "w_key": bell_draw(key_list[6], (D, HEADS * HD), D ** -0.5, 0.1875),
        "w_value": bell_draw(key_list[7], (D, HEADS * HD), D ** -0.5, 0.1875),
    }


NEG_FILL = -1e+30
EPSILON = 1e-06

def normalize(source_rows):
    wide_rows = source_rows.astype(jnp.float32)
    factor = lax.rsqrt(lax.optimization_barrier(jnp.mean(wide_rows * wide_rows, axis=-1, keepdims=True)) + EPSILON)
    return (wide_rows * factor).astype(jnp.bfloat16)

def reference(prefix, keep_blocks, keep_count, latent_inputs, latent_pos, w_query, w_key, w_value):
    latents = LAT_DEV * N_CTX
    order_ids = jnp.arange(BLK_DEV, dtype=jnp.int32)
    matched = (keep_blocks[:, :, :, None] == order_ids[None, None, None, :]) & (order_ids[None, None, :, None] < keep_count[:, :, None, None])
    kept_grid = jnp.any(matched, axis=2)
    kept_flat = jnp.transpose(kept_grid, (1, 0, 2)).reshape(-1)
    kept_total = N_CTX * N_HEAD * (BLK_DEV // 2)
    block_ids = jnp.nonzero(kept_flat, size=kept_total)[0].astype(jnp.int32)
    all_blocks = prefix.reshape(N_CTX * N_HEAD * BLK_DEV, BLOCK, D)
    kept_rows = jnp.take(all_blocks, block_ids, axis=0).reshape(kept_total * BLOCK, D)
    key_pos = (block_ids[:, None] * BLOCK + jnp.arange(BLOCK, dtype=jnp.int32)[None, :]).reshape(-1)
    normed = normalize(kept_rows)
    key_all = jnp.dot(normed, w_key, preferred_element_type=jnp.float32).astype(jnp.bfloat16)
    value_all = jnp.dot(normed, w_value, preferred_element_type=jnp.float32).astype(jnp.bfloat16)
    latent_normed = normalize(latent_inputs)
    query = (jnp.dot(latent_normed, w_query, preferred_element_type=jnp.float32) * HD ** (-0.5)).astype(jnp.bfloat16)
    self_key = jnp.dot(latent_normed, w_key, preferred_element_type=jnp.float32).astype(jnp.bfloat16)
    self_value = jnp.dot(latent_normed, w_value, preferred_element_type=jnp.float32).astype(jnp.bfloat16)
    self_score = lax.optimization_barrier(jnp.sum((query.astype(jnp.float32) * self_key.astype(jnp.float32)).reshape(latents, HEADS, HD), axis=2))
    block_rows = min(512, latents)
    block_count = latents // block_rows
    key_count = kept_total * BLOCK
    key_heads = key_all.reshape(key_count, HEADS, HD).transpose(1, 0, 2)
    value_heads = value_all.reshape(key_count, HEADS, HD).transpose(1, 0, 2)
    query_heads = query.reshape(block_count, block_rows, HEADS, HD).transpose(2, 0, 1, 3)
    self_scores = self_score.reshape(block_count, block_rows, HEADS).transpose(2, 0, 1)
    self_values = self_value.reshape(block_count, block_rows, HEADS, HD).transpose(2, 0, 1, 3)
    pos_blocks = latent_pos.reshape(block_count, block_rows)

    def per_head(head_args):
        key_head, value_head, query_head, score_head, svalue_head = head_args

        def per_block(block_args):
            query_block, pos_block, sscore_block, svalue_block = block_args
            scores = jnp.dot(query_block, key_head.T, preferred_element_type=jnp.float32)
            allowed = key_pos[None, :] < pos_block[:, None]
            masked = jnp.where(allowed, scores, NEG_FILL)
            row_top = jnp.maximum(lax.optimization_barrier(jnp.max(masked, axis=1)), sscore_block)
            weights = jnp.where(allowed, jnp.exp(masked - row_top[:, None]), 0.0)
            self_weight = jnp.exp(sscore_block - row_top)
            denominator = lax.optimization_barrier(jnp.sum(weights, axis=1)) + self_weight
            numerator = jnp.dot(weights.astype(jnp.bfloat16), value_head, preferred_element_type=jnp.float32)
            numerator = numerator + self_weight[:, None] * svalue_block.astype(jnp.float32)
            return (numerator / denominator[:, None]).astype(jnp.bfloat16)
        return lax.map(per_block, (query_head, pos_blocks, score_head, svalue_head))
    results = lax.map(per_head, (key_heads, value_heads, query_heads, self_scores, self_values))
    return results.transpose(1, 2, 0, 3).reshape(latents, HEADS * HD)
```

```python
import functools

import jax
import jax.numpy as jnp
from jax import lax
from jax.experimental import pallas as pl
from jax.experimental.pallas import tpu as pltpu
from jax.sharding import PartitionSpec as P

HD = 64
BLOCK = 128
PAIR = 2 * HD
LANES = 128

PROJECT_ROWS = 512
AHEAD = 2
WEIGHT_PARTS = 1
ATTEND_ROWS = 256
ATTEND_GRANT = 57 * 2**20
VMEM_GRANT = 12 * 2**20

NEG_FILL = -1e30
EPSILON = 1e-06

FAR = 2**30

NT = (((1,), (1,)), ((), ()))


def normalize(source_rows):
    wide_rows = source_rows.astype(jnp.float32)
    factor = lax.rsqrt(jnp.mean(wide_rows * wide_rows, axis=-1, keepdims=True) + EPSILON)
    return (wide_rows * factor).astype(jnp.bfloat16)

VMEM = pl.BlockSpec(memory_space=pltpu.VMEM)
SMEM = pl.BlockSpec(memory_space=pltpu.SMEM)
HBM = pl.BlockSpec(memory_space=pltpu.HBM)


def query_kernel(latent_hbm, w_query_hbm, out_hbm, latent_ref, w_query_ref, query_ref, in_sem, out_sem):
    latent_copy = pltpu.make_async_copy(latent_hbm, latent_ref, in_sem.at[0])
    weight_copy = pltpu.make_async_copy(w_query_hbm, w_query_ref, in_sem.at[1])
    weight_copy.start()
    latent_copy.start()
    latent_copy.wait()
    normed = normalize(latent_ref[...])
    weight_copy.wait()
    query = jnp.dot(normed, w_query_ref[...], preferred_element_type=jnp.float32) * HD ** (-0.5)
    query_ref[...] = query.astype(jnp.bfloat16)
    copies = [
        pltpu.make_async_copy(query_ref, out_hbm.at[k], out_sem.at[k])
        for k in range(out_hbm.shape[0])
    ]
    for copy in copies:
        copy.start()
    for copy in copies:
        copy.wait()


def self_kernel(
    after_hbm, latent_ref, query_hbm, w_key_hbm, w_value_hbm, score_ref, value_ref, query_ref, key_ref, column_ref, sem
):
    latent_rows, width = query_ref.shape
    mine = pl.ds(pl.multiple_of(lax.axis_index("head") * width, width), width)
    query_copy = pltpu.make_async_copy(query_hbm.at[0], query_ref, sem.at[0])
    key_copy = pltpu.make_async_copy(w_key_hbm.at[:, mine], key_ref, sem.at[1])
    value_copy = pltpu.make_async_copy(w_value_hbm.at[:, mine], column_ref, sem.at[2])
    query_copy.start()
    key_copy.start()
    value_copy.start()
    normed = normalize(latent_ref[...])
    key_copy.wait()
    key = jnp.dot(normed, key_ref[...], preferred_element_type=jnp.float32).astype(jnp.bfloat16)
    query_copy.wait()
    products = query_ref[...].astype(jnp.float32) * key.astype(jnp.float32)
    for first in range(0, width, HD):
        score = jnp.sum(products[:, first : first + HD], axis=1, keepdims=True)
        score_ref[:, first : first + HD] = jnp.broadcast_to(score, (latent_rows, HD))
    value_copy.wait()
    value = jnp.dot(normed, column_ref[...], preferred_element_type=jnp.float32)
    value_ref[...] = value.astype(jnp.bfloat16)


def project_kernel(
    prefix_hbm, w_key_hbm, w_value_hbm, both_hbm, prefix_ref, w_key_ref, w_value_ref, both_ref, in_sem, out_sem, *, tile
):
    rows = prefix_ref.shape[0]
    pairs = both_ref.shape[1]
    row_copies = [
        pltpu.make_async_copy(
            prefix_hbm.at[pl.ds(r, tile)], prefix_ref.at[pl.ds(r, tile)], in_sem.at[r // tile]
        )
        for r in range(0, rows, tile)
    ]
    columns = w_key_ref.shape[1]
    width = columns // WEIGHT_PARTS

    def part_copies(hbm, ref, first):
        return [
            pltpu.make_async_copy(
                hbm.at[:, pl.ds(k * width, width)], ref.at[:, pl.ds(k * width, width)], in_sem.at[first + k]
            )
            for k in range(WEIGHT_PARTS)
        ]

    def project_rows(normed, ref, waits):
        parts = []
        for k in range(WEIGHT_PARTS):
            if waits:
                waits[k].wait()
            part = jnp.dot(
                normed, ref[:, k * width : (k + 1) * width], preferred_element_type=jnp.float32
            )
            parts.append(part.astype(jnp.bfloat16))
        return jnp.concatenate(parts, axis=1)

    first = rows // tile
    key_copies = part_copies(w_key_hbm, w_key_ref, first)
    value_copies = part_copies(w_value_hbm, w_value_ref, first + WEIGHT_PARTS)
    row_copies[0].start()
    for copy in key_copies + value_copies + row_copies[1:]:
        copy.start()
    out_copies = []
    for r in range(0, rows, tile):
        span = pl.ds(r, tile)
        k = r // tile
        row_copies[k].wait()
        normed = normalize(prefix_ref[r : r + tile, :])
        key = project_rows(normed, w_key_ref, key_copies if r == 0 else None)
        for p in range(pairs):
            both_ref[0, p, r : r + tile, :] = key[:, p * PAIR : (p + 1) * PAIR]
        copy = pltpu.make_async_copy(both_ref.at[0, :, span, :], both_hbm.at[0, :, span, :], out_sem.at[2 * k])
        copy.start()
        out_copies.append(copy)
        value = project_rows(normed, w_value_ref, value_copies if r == 0 else None)
        for p in range(pairs):
            for b in range(r, r + tile, BLOCK):
                both_ref[1, p, b : b + BLOCK, :] = value[b - r : b - r + BLOCK, p * PAIR : (p + 1) * PAIR].T
        copy = pltpu.make_async_copy(
            both_ref.at[1, :, span, :], both_hbm.at[1, :, span, :], out_sem.at[2 * k + 1]
        )
        copy.start()
        out_copies.append(copy)
    for copy in out_copies:
        copy.wait()


def attend_kernel(
    list_hbm, count_hbm, pos_hbm, query_ref, both_hbm, out_ref,
    list_ref, count_ref, pos_ref, start_ref, bias_ref, both_ref, even_ref, odd_ref, log_ref, small_sem, sem, *, chunk
):
    _, pairs, rows, _ = both_ref.shape
    tiles = bias_ref.shape[0]
    blocks = rows // BLOCK

    def fetch(pair):
        return (
            pltpu.make_async_copy(both_hbm.at[0, pair], both_ref.at[0, pair], sem.at[0, pair]),
            pltpu.make_async_copy(both_hbm.at[1, pair], both_ref.at[1, pair], sem.at[1, pair]),
        )

    small_copies = [
        pltpu.make_async_copy(list_hbm, list_ref, small_sem.at[0]),
        pltpu.make_async_copy(count_hbm, count_ref, small_sem.at[1]),
        pltpu.make_async_copy(pos_hbm, pos_ref, small_sem.at[2]),
    ]
    for copy in small_copies:
        copy.start()
    for p in range(min(AHEAD, pairs)):
        for copy in fetch(p):
            copy.start()
    for copy in small_copies:
        copy.wait()

    shard = lax.axis_index("ctx") * lax.axis_size("head") + lax.axis_index("head")
    for b in range(blocks):
        start_ref[b] = FAR
    for j in range(blocks):
        block = list_ref[0, 0, j]

        @pl.when(j < count_ref[0, 0])
        def _():
            start_ref[block] = (shard * blocks + block) * BLOCK

    row_iota = lax.broadcasted_iota(jnp.int32, (BLOCK, LANES), 0)
    for t in range(tiles):
        pos = pos_ref[:, t * LANES : (t + 1) * LANES]
        for b in range(blocks):
            allowed = row_iota < pos - start_ref[b]
            bias_ref[t, b * BLOCK : (b + 1) * BLOCK, :] = jnp.where(allowed, 0.0, NEG_FILL)

    ctx_count, head_count, latent_rows, head_width = query_ref.shape
    ctx_tile = LANES // latent_rows
    per_head = head_width // PAIR
    heads_here = head_width // HD
    steps = tiles * pairs
    half = lax.broadcasted_iota(jnp.int32, (LANES, PAIR), 1) < HD

    def place(step):
        tile, pair = step // pairs, step % pairs
        return tile, pair, pair // per_head, pair % per_head

    def spread_of(step):
        tile, _, group, j = place(step)
        query = query_ref[
            pl.ds(tile * ctx_tile, ctx_tile), group, :, pl.ds(pl.multiple_of(j * PAIR, PAIR), PAIR)
        ].reshape(LANES, PAIR)
        zero = jnp.zeros_like(query)
        return jnp.concatenate([jnp.where(half, query, zero), jnp.where(half, zero, query)], axis=0)

    def score_part(step, spread, r, store_ref, top8):
        tile, pair, _, _ = place(step)
        scores = lax.dot_general(
            both_ref[0, pair, r : r + chunk, :], spread, NT, preferred_element_type=jnp.float32
        )
        bias = bias_ref[tile, r : r + chunk, :]
        scores = scores + jnp.concatenate([bias, bias], axis=1)
        store_ref[r : r + chunk, :] = scores
        return jnp.maximum(top8, jnp.max(scores.reshape(chunk // 8, 8, 2 * LANES), axis=0))

    def weigh_part(step, r, load_ref, top, sum8, total):
        pair = place(step)[1]
        weights = jnp.exp(load_ref[r : r + chunk, :] - top)
        sum8 = sum8 + jnp.sum(weights.reshape(chunk // 8, 8, 2 * LANES), axis=0)
        values = [both_ref[1, pair, b : b + BLOCK, :] for b in range(r, r + chunk, BLOCK)]
        total = total + jnp.dot(
            jnp.concatenate(values, axis=1),
            weights.astype(jnp.bfloat16),
            preferred_element_type=jnp.float32,
        )
        return sum8, total

    def finish(step, top, sum8, total):
        tile, pair, group, j = place(step)
        sums = jnp.sum(sum8, axis=0, keepdims=True)
        scaled = total / sums
        own = jnp.concatenate([scaled[:HD, :LANES], scaled[HD:, LANES:]], axis=0)
        out_ref[
            pl.ds(tile * ctx_tile, ctx_tile),
            group,
            pl.ds(pl.multiple_of(j * latent_rows, latent_rows), latent_rows),
            :,
        ] = own.T.astype(jnp.bfloat16).reshape(ctx_tile, latent_rows, PAIR)
        log_sum = top + jnp.log(sums)
        log_ref[step] = jnp.concatenate([log_sum[:, :LANES], log_sum[:, LANES:]], axis=0)

    lowest = jnp.full((8, 2 * LANES), NEG_FILL, jnp.float32)
    none = jnp.zeros((8, 2 * LANES), jnp.float32)
    empty = jnp.zeros((PAIR, 2 * LANES), jnp.float32)
    chunks = range(0, rows, chunk)

    def arrive(step):
        @pl.when(step < pairs)
        def _():
            for copy in fetch(step):
                copy.wait()

        @pl.when(step + AHEAD < pairs)
        def _():
            for copy in fetch(step + AHEAD):
                copy.start()

    def both(step, store_ref, load_ref, top):
        arrive(step)
        spread = spread_of(step)
        top8, sum8, total = lowest, none, empty
        for r in chunks:
            top8 = score_part(step, spread, r, store_ref, top8)
            sum8, total = weigh_part(step - 1, r, load_ref, top, sum8, total)
        finish(step - 1, top, sum8, total)
        return jnp.max(top8, axis=0, keepdims=True)

    arrive(0)
    spread = spread_of(0)
    top8 = lowest
    for r in chunks:
        top8 = score_part(0, spread, r, even_ref, top8)
    top = jnp.max(top8, axis=0, keepdims=True)

    def turn(k, top):
        top = both(2 * k + 1, odd_ref, even_ref, top)
        return both(2 * k + 2, even_ref, odd_ref, top)

    top = lax.fori_loop(0, steps // 2 - 1, turn, top)
    top = both(steps - 1, odd_ref, even_ref, top)
    sum8, total = none, empty
    for r in chunks:
        sum8, total = weigh_part(steps - 1, r, odd_ref, top, sum8, total)
    finish(steps - 1, top, sum8, total)

    data_rows = per_head * latent_rows
    for tile in range(tiles):
        for group in range(head_count):
            logs = jnp.concatenate(
                [log_ref[tile * pairs + group * per_head + j] for j in range(per_head)], axis=0
            )
            high = logs.astype(jnp.bfloat16)
            low = logs - high.astype(jnp.float32)
            pieces = jnp.concatenate([high.astype(jnp.float32), low], axis=0).astype(jnp.bfloat16)
            for c in range(ctx_tile):
                out_ref[tile * ctx_tile + c, group, data_rows : data_rows + 2 * heads_here, :] = pieces


def project(prefix, w_key, w_value):
    rows, model = prefix.shape
    columns = w_key.shape[1]
    pairs = columns // PAIR
    small = prefix.dtype
    return pl.pallas_call(
        functools.partial(project_kernel, tile=PROJECT_ROWS),
        in_specs=[HBM] * 3,
        out_specs=HBM,
        out_shape=jax.ShapeDtypeStruct((2, pairs, rows, PAIR), small),
        scratch_shapes=[
            pltpu.VMEM(prefix.shape, small),
            pltpu.VMEM(w_key.shape, small),
            pltpu.VMEM(w_value.shape, small),
            pltpu.VMEM((2, pairs, rows, PAIR), small),
            pltpu.SemaphoreType.DMA((2 * WEIGHT_PARTS + rows // PROJECT_ROWS,)),
            pltpu.SemaphoreType.DMA((2 * (rows // PROJECT_ROWS),)),
        ],
        cost_estimate=pl.CostEstimate(
            flops=4 * rows * model * columns,
            bytes_accessed=2 * (rows * model + 2 * model * columns + 2 * rows * columns),
            transcendentals=0,
        ),
        name="project",
    )(prefix, w_key, w_value)


def attend(keep_blocks, keep_count, latent_pos, queries, both):
    ctx_count, head_count, latent_rows, head_width = queries.shape
    _, pairs, rows, _ = both.shape
    columns = pairs * PAIR
    latents = latent_pos.shape[0]
    tiles = latents // LANES
    heads_here = head_width // HD
    small = queries.dtype
    packed_rows = latent_rows * head_width // LANES + 2 * heads_here
    return pl.pallas_call(
        functools.partial(attend_kernel, chunk=ATTEND_ROWS),
        in_specs=[HBM, HBM, HBM, VMEM, HBM],
        out_specs=VMEM,
        out_shape=jax.ShapeDtypeStruct((ctx_count, head_count, packed_rows, LANES), small),
        scratch_shapes=[
            pltpu.SMEM(keep_blocks.shape, jnp.int32),
            pltpu.SMEM(keep_count.shape, jnp.int32),
            pltpu.VMEM((1, latents), jnp.int32),
            pltpu.SMEM((rows // BLOCK,), jnp.int32),
            pltpu.VMEM((tiles, rows, LANES), jnp.float32),
            pltpu.VMEM((2, pairs, rows, PAIR), small),
            pltpu.VMEM((rows, 2 * LANES), jnp.float32),
            pltpu.VMEM((rows, 2 * LANES), jnp.float32),
            pltpu.VMEM((tiles * pairs, 2, LANES), jnp.float32),
            pltpu.SemaphoreType.DMA((3,)),
            pltpu.SemaphoreType.DMA((2, pairs)),
        ],
        compiler_params=pltpu.CompilerParams(vmem_limit_bytes=ATTEND_GRANT),
        cost_estimate=pl.CostEstimate(
            flops=16 * rows * columns * latents,
            bytes_accessed=4 * rows * columns,
            transcendentals=rows * columns * latents // HD,
        ),
        name="attend",
    )(keep_blocks, keep_count, latent_pos.reshape(1, latents), queries, both)


def join_kernel(parts_ref, self_score_ref, self_value_ref, out_ref, turned_ref):
    sources = parts_ref.shape[0]
    latent_rows, width = out_ref.shape
    heads = width // HD
    per_head = width // PAIR
    data_rows = per_head * latent_rows
    wide = parts_ref[:, data_rows:, :].astype(jnp.float32)
    logs = wide + pltpu.roll(wide, heads, 1)
    top = jnp.max(logs, axis=0)
    weights = jnp.exp(logs - top[None])
    sums = jnp.sum(weights, axis=0)
    turned_ref[:, : sources * 8] = weights.reshape(sources * 8, LANES).T
    filler = jnp.zeros((LANES - 16, LANES), jnp.float32)
    turned_ref[:, sources * 8 :] = jnp.concatenate([top, sums, filler], axis=0).T
    lane = (lax.axis_index("ctx") * latent_rows) % LANES
    mine = turned_ref[pl.ds(pl.multiple_of(lane, 8), latent_rows), :]
    half = lax.broadcasted_iota(jnp.int32, (latent_rows, PAIR), 1) < HD

    def widen(first):
        left = jnp.broadcast_to(mine[:, first : first + 1], (latent_rows, PAIR))
        right = jnp.broadcast_to(mine[:, first + 1 : first + 2], (latent_rows, PAIR))
        return jnp.where(half, left, right)

    for j in range(per_head):
        columns = slice(j * PAIR, (j + 1) * PAIR)
        total = jnp.zeros((latent_rows, PAIR), jnp.float32)
        for s in range(sources):
            part = parts_ref[s, j * latent_rows : (j + 1) * latent_rows, :].astype(jnp.float32)
            total = total + widen(8 * s + 2 * j) * part
        kept_top = widen(8 * sources + 2 * j)
        kept_sum = widen(8 * sources + 8 + 2 * j)
        self_score = self_score_ref[:, columns]
        final_top = jnp.maximum(kept_top, self_score)
        keep = jnp.exp(kept_top - final_top)
        self_weight = jnp.exp(self_score - final_top)
        denominator = kept_sum * keep + self_weight
        numerator = total * keep + self_weight * self_value_ref[:, columns].astype(jnp.float32)
        out_ref[:, columns] = (numerator / denominator).astype(jnp.bfloat16)


def per_device(prefix, keep_blocks, keep_count, latent_inputs, latent_pos, w_query, w_key, w_value):
    head_count = lax.axis_size("head")
    ctx_count = lax.axis_size("ctx")
    device_count = head_count * ctx_count
    head_width = w_query.shape[1]
    model = prefix.shape[1]
    latent_rows = latent_inputs.shape[0]
    axes = ("ctx", "head")
    small = jnp.bfloat16

    copies = pl.pallas_call(
        query_kernel,
        in_specs=[HBM] * 2,
        out_specs=HBM,
        out_shape=jax.ShapeDtypeStruct((device_count, latent_rows, head_width), small),
        scratch_shapes=[
            pltpu.VMEM(latent_inputs.shape, small),
            pltpu.VMEM(w_query.shape, small),
            pltpu.VMEM((latent_rows, head_width), small),
            pltpu.SemaphoreType.DMA((2,)),
            pltpu.SemaphoreType.DMA((device_count,)),
        ],
        name="query",
    )(latent_inputs, w_query)
    queries = lax.all_to_all(copies, axes, split_axis=0, concat_axis=0, tiled=True)
    queries = queries.reshape(ctx_count, head_count, latent_rows, head_width)

    both = project(prefix, w_key, w_value)
    packed = attend(keep_blocks, keep_count, latent_pos, queries, both)
    packed_rows = packed.shape[2]
    arrived = lax.all_to_all(
        packed.reshape(device_count, packed_rows, LANES), axes, split_axis=0, concat_axis=0, tiled=True
    )

    self_score, self_value = pl.pallas_call(
        self_kernel,
        in_specs=[HBM, VMEM, HBM, HBM, HBM],
        out_specs=[VMEM] * 2,
        out_shape=[
            jax.ShapeDtypeStruct((latent_rows, head_width), jnp.float32),
            jax.ShapeDtypeStruct((latent_rows, head_width), small),
        ],
        scratch_shapes=[
            pltpu.VMEM((latent_rows, head_width), small),
            pltpu.VMEM((model, head_width), small),
            pltpu.VMEM((model, head_width), small),
            pltpu.SemaphoreType.DMA((3,)),
        ],
        compiler_params=pltpu.CompilerParams(vmem_limit_bytes=VMEM_GRANT),
        cost_estimate=pl.CostEstimate(
            flops=4 * latent_rows * model * head_width,
            bytes_accessed=4 * model * head_width,
            transcendentals=0,
        ),
        name="own",
    )(packed, latent_inputs, copies, w_key, w_value)

    return pl.pallas_call(
        join_kernel,
        in_specs=[VMEM] * 3,
        out_specs=VMEM,
        out_shape=jax.ShapeDtypeStruct((latent_rows, head_width), small),
        scratch_shapes=[pltpu.VMEM((LANES, device_count * 8 + LANES), jnp.float32)],
        compiler_params=pltpu.CompilerParams(vmem_limit_bytes=VMEM_GRANT),
        name="join",
    )(arrived, self_score, self_value)


def solution(mesh):
    return jax.shard_map(
        per_device,
        mesh=mesh,
        in_specs=(
            P(("ctx", "head"), None),
            P("head", "ctx", None),
            P("head", "ctx"),
            P("ctx", None),
            P(),
            P(None, "head"),
            P(),
            P(),
        ),
        out_specs=P("ctx", "head"),
        check_vma=False,
    )
```

```python
import functools

import jax
import jax.numpy as jnp
from jax import lax
from jax.experimental import pallas as pl
from jax.experimental.pallas import tpu as pltpu
from jax.sharding import PartitionSpec as P

HD = 64
BLOCK = 128
PAIR = 2 * HD
LANES = 128

PROJECT_ROWS = 512
AHEAD = 2
WEIGHT_PARTS = 1
ATTEND_ROWS = 256
ATTEND_GRANT = 50 * 2**20
VMEM_GRANT = 12 * 2**20

NEG_FILL = -1e30
EPSILON = 1e-06

FAR = 2**30

NT = (((1,), (1,)), ((), ()))


def normalize(source_rows):
    wide_rows = source_rows.astype(jnp.float32)
    factor = lax.rsqrt(jnp.mean(wide_rows * wide_rows, axis=-1, keepdims=True) + EPSILON)
    return (wide_rows * factor).astype(jnp.bfloat16)

VMEM = pl.BlockSpec(memory_space=pltpu.VMEM)
SMEM = pl.BlockSpec(memory_space=pltpu.SMEM)
HBM = pl.BlockSpec(memory_space=pltpu.HBM)


def query_kernel(latent_hbm, w_query_hbm, out_hbm, latent_ref, w_query_ref, query_ref, in_sem, out_sem):
    latent_copy = pltpu.make_async_copy(latent_hbm, latent_ref, in_sem.at[0])
    weight_copy = pltpu.make_async_copy(w_query_hbm, w_query_ref, in_sem.at[1])
    weight_copy.start()
    latent_copy.start()
    latent_copy.wait()
    normed = normalize(latent_ref[...])
    weight_copy.wait()
    query = jnp.dot(normed, w_query_ref[...], preferred_element_type=jnp.float32) * HD ** (-0.5)
    query_ref[...] = query.astype(jnp.bfloat16)
    copies = [
        pltpu.make_async_copy(query_ref, out_hbm.at[k], out_sem.at[k])
        for k in range(out_hbm.shape[0])
    ]
    for copy in copies:
        copy.start()
    for copy in copies:
        copy.wait()


def self_kernel(
    after_hbm, latent_ref, query_hbm, w_key_hbm, w_value_hbm, score_ref, value_ref, query_ref, key_ref, column_ref, sem
):
    latent_rows, width = query_ref.shape
    mine = pl.ds(pl.multiple_of(lax.axis_index("head") * width, width), width)
    query_copy = pltpu.make_async_copy(query_hbm.at[0], query_ref, sem.at[0])
    key_copy = pltpu.make_async_copy(w_key_hbm.at[:, mine], key_ref, sem.at[1])
    value_copy = pltpu.make_async_copy(w_value_hbm.at[:, mine], column_ref, sem.at[2])
    query_copy.start()
    key_copy.start()
    value_copy.start()
    normed = normalize(latent_ref[...])
    key_copy.wait()
    key = jnp.dot(normed, key_ref[...], preferred_element_type=jnp.float32).astype(jnp.bfloat16)
    query_copy.wait()
    products = query_ref[...].astype(jnp.float32) * key.astype(jnp.float32)
    for first in range(0, width, HD):
        score = jnp.sum(products[:, first : first + HD], axis=1, keepdims=True)
        score_ref[:, first : first + HD] = jnp.broadcast_to(score, (latent_rows, HD))
    value_copy.wait()
    value = jnp.dot(normed, column_ref[...], preferred_element_type=jnp.float32)
    value_ref[...] = value.astype(jnp.bfloat16)


def project_kernel(
    prefix_hbm, w_key_hbm, w_value_hbm, both_hbm, prefix_ref, w_key_ref, w_value_ref, both_ref, in_sem, out_sem, *, tile
):
    rows = prefix_ref.shape[0]
    pairs = both_ref.shape[1]
    row_copies = [
        pltpu.make_async_copy(
            prefix_hbm.at[pl.ds(r, tile)], prefix_ref.at[pl.ds(r, tile)], in_sem.at[r // tile]
        )
        for r in range(0, rows, tile)
    ]
    columns = w_key_ref.shape[1]
    width = columns // WEIGHT_PARTS

    def part_copies(hbm, ref, first):
        return [
            pltpu.make_async_copy(
                hbm.at[:, pl.ds(k * width, width)], ref.at[:, pl.ds(k * width, width)], in_sem.at[first + k]
            )
            for k in range(WEIGHT_PARTS)
        ]

    def project_rows(normed, ref, waits):
        parts = []
        for k in range(WEIGHT_PARTS):
            if waits:
                waits[k].wait()
            part = jnp.dot(
                normed, ref[:, k * width : (k + 1) * width], preferred_element_type=jnp.float32
            )
            parts.append(part.astype(jnp.bfloat16))
        return jnp.concatenate(parts, axis=1)

    first = rows // tile
    key_copies = part_copies(w_key_hbm, w_key_ref, first)
    value_copies = part_copies(w_value_hbm, w_value_ref, first + WEIGHT_PARTS)
    row_copies[0].start()
    for copy in key_copies + value_copies + row_copies[1:]:
        copy.start()
    out_copies = []
    for r in range(0, rows, tile):
        span = pl.ds(r, tile)
        k = r // tile
        row_copies[k].wait()
        normed = normalize(prefix_ref[r : r + tile, :])
        key = project_rows(normed, w_key_ref, key_copies if r == 0 else None)
        for p in range(pairs):
            both_ref[0, p, r : r + tile, :] = key[:, p * PAIR : (p + 1) * PAIR]
        copy = pltpu.make_async_copy(both_ref.at[0, :, span, :], both_hbm.at[0, :, span, :], out_sem.at[2 * k])
        copy.start()
        out_copies.append(copy)
        value = project_rows(normed, w_value_ref, value_copies if r == 0 else None)
        for p in range(pairs):
            for b in range(r, r + tile, BLOCK):
                both_ref[1, p, b : b + BLOCK, :] = value[b - r : b - r + BLOCK, p * PAIR : (p + 1) * PAIR].T
        copy = pltpu.make_async_copy(
            both_ref.at[1, :, span, :], both_hbm.at[1, :, span, :], out_sem.at[2 * k + 1]
        )
        copy.start()
        out_copies.append(copy)
    for copy in out_copies:
        copy.wait()


def attend_kernel(
    count_ref, pos_ref, query_ref, list_hbm, both_hbm, out_hbm,
    list_ref, bias_ref, both_ref, even_ref, odd_ref, log_ref, out_ref, list_sem, sem, out_sem, *, chunk
):
    _, pairs, rows, _ = both_ref.shape
    tiles = bias_ref.shape[0]
    blocks = rows // BLOCK

    def fetch(pair):
        return (
            pltpu.make_async_copy(both_hbm.at[0, pair], both_ref.at[0, pair], sem.at[0, pair]),
            pltpu.make_async_copy(both_hbm.at[1, pair], both_ref.at[1, pair], sem.at[1, pair]),
        )

    list_copy = pltpu.make_async_copy(list_hbm, list_ref, list_sem)
    list_copy.start()
    for p in range(min(AHEAD, pairs)):
        for copy in fetch(p):
            copy.start()
    shard = lax.axis_index("ctx") * lax.axis_size("head") + lax.axis_index("head")
    count = jnp.broadcast_to(count_ref[...], (BLOCK, LANES))
    row_iota = lax.broadcasted_iota(jnp.int32, (BLOCK, LANES), 0)
    list_copy.wait()
    for j in range(blocks):
        block = list_ref[0, 0, j]
        span = pl.ds(pl.multiple_of(block * BLOCK, BLOCK), BLOCK)
        start = (shard * blocks + block) * BLOCK
        for t in range(tiles):
            pos = pos_ref[:, t * LANES : (t + 1) * LANES]
            allowed = jnp.logical_and(row_iota < pos - start, count > j)
            bias_ref[t, span, :] = jnp.where(allowed, 0.0, NEG_FILL)
    ctx_count, head_count, latent_rows, head_width = query_ref.shape
    ctx_tile = LANES // latent_rows
    per_head = head_width // PAIR
    heads_here = head_width // HD
    steps = tiles * pairs
    half = lax.broadcasted_iota(jnp.int32, (LANES, PAIR), 1) < HD

    data_rows = per_head * latent_rows

    def send(tile, group):
        span = pl.ds(tile * ctx_tile, ctx_tile)
        return pltpu.make_async_copy(
            out_ref.at[span, group], out_hbm.at[span, group], out_sem.at[tile, group]
        )

    def place(step):
        tile, pair = step // pairs, step % pairs
        return tile, pair, pair // per_head, pair % per_head

    def spread_of(step):
        tile, _, group, j = place(step)
        query = query_ref[
            pl.ds(tile * ctx_tile, ctx_tile), group, :, pl.ds(pl.multiple_of(j * PAIR, PAIR), PAIR)
        ].reshape(LANES, PAIR)
        zero = jnp.zeros_like(query)
        return jnp.concatenate([jnp.where(half, query, zero), jnp.where(half, zero, query)], axis=0)

    def score_part(step, spread, r, store_ref, top8):
        tile, pair, _, _ = place(step)
        scores = lax.dot_general(
            both_ref[0, pair, r : r + chunk, :], spread, NT, preferred_element_type=jnp.float32
        )
        bias = bias_ref[tile, r : r + chunk, :]
        scores = scores + jnp.concatenate([bias, bias], axis=1)
        store_ref[r : r + chunk, :] = scores
        return jnp.maximum(top8, jnp.max(scores.reshape(chunk // 8, 8, 2 * LANES), axis=0))

    def weigh_part(step, r, load_ref, top, sum8, total):
        pair = place(step)[1]
        weights = jnp.exp(load_ref[r : r + chunk, :] - top)
        sum8 = sum8 + jnp.sum(weights.reshape(chunk // 8, 8, 2 * LANES), axis=0)
        values = [both_ref[1, pair, b : b + BLOCK, :] for b in range(r, r + chunk, BLOCK)]
        total = total + jnp.dot(
            jnp.concatenate(values, axis=1),
            weights.astype(jnp.bfloat16),
            preferred_element_type=jnp.float32,
        )
        return sum8, total

    def finish(step, top, sum8, total):
        tile, pair, group, j = place(step)
        sums = jnp.sum(sum8, axis=0, keepdims=True)
        scaled = total / sums
        own = jnp.concatenate([scaled[:HD, :LANES], scaled[HD:, LANES:]], axis=0)
        out_ref[
            pl.ds(tile * ctx_tile, ctx_tile),
            group,
            pl.ds(pl.multiple_of(j * latent_rows, latent_rows), latent_rows),
            :,
        ] = own.T.astype(jnp.bfloat16).reshape(ctx_tile, latent_rows, PAIR)
        log_sum = top + jnp.log(sums)
        log_ref[j] = jnp.concatenate([log_sum[:, :LANES], log_sum[:, LANES:]], axis=0)

    def depart(step):
        tile, _, group, j = place(step)

        @pl.when(j == per_head - 1)
        def _():
            logs = jnp.concatenate([log_ref[k] for k in range(per_head)], axis=0)
            high = logs.astype(jnp.bfloat16)
            low = logs - high.astype(jnp.float32)
            pieces = jnp.concatenate([high.astype(jnp.float32), low], axis=0).astype(jnp.bfloat16)
            for c in range(ctx_tile):
                out_ref[tile * ctx_tile + c, group, data_rows : data_rows + 2 * heads_here, :] = pieces
            send(tile, group).start()

    lowest = jnp.full((8, 2 * LANES), NEG_FILL, jnp.float32)
    none = jnp.zeros((8, 2 * LANES), jnp.float32)
    empty = jnp.zeros((PAIR, 2 * LANES), jnp.float32)
    chunks = range(0, rows, chunk)

    def arrive(step):
        @pl.when(step < pairs)
        def _():
            for copy in fetch(step):
                copy.wait()

        @pl.when(step + AHEAD < pairs)
        def _():
            for copy in fetch(step + AHEAD):
                copy.start()

    def both(step, store_ref, load_ref, top):
        arrive(step)
        spread = spread_of(step)
        top8, sum8, total = lowest, none, empty
        for r in chunks:
            top8 = score_part(step, spread, r, store_ref, top8)
            sum8, total = weigh_part(step - 1, r, load_ref, top, sum8, total)
        finish(step - 1, top, sum8, total)
        depart(step - 1)
        return jnp.max(top8, axis=0, keepdims=True)

    arrive(0)
    spread = spread_of(0)
    top8 = lowest
    for r in chunks:
        top8 = score_part(0, spread, r, even_ref, top8)
    top = jnp.max(top8, axis=0, keepdims=True)

    def turn(k, top):
        top = both(2 * k + 1, odd_ref, even_ref, top)
        return both(2 * k + 2, even_ref, odd_ref, top)

    top = lax.fori_loop(0, steps // 2 - 1, turn, top)
    top = both(steps - 1, odd_ref, even_ref, top)
    sum8, total = none, empty
    for r in chunks:
        sum8, total = weigh_part(steps - 1, r, odd_ref, top, sum8, total)
    finish(steps - 1, top, sum8, total)
    depart(steps - 1)

    for tile in range(tiles):
        for group in range(head_count):
            send(tile, group).wait()


def project(prefix, w_key, w_value):
    rows, model = prefix.shape
    columns = w_key.shape[1]
    pairs = columns // PAIR
    small = prefix.dtype
    return pl.pallas_call(
        functools.partial(project_kernel, tile=PROJECT_ROWS),
        in_specs=[HBM] * 3,
        out_specs=HBM,
        out_shape=jax.ShapeDtypeStruct((2, pairs, rows, PAIR), small),
        scratch_shapes=[
            pltpu.VMEM(prefix.shape, small),
            pltpu.VMEM(w_key.shape, small),
            pltpu.VMEM(w_value.shape, small),
            pltpu.VMEM((2, pairs, rows, PAIR), small),
            pltpu.SemaphoreType.DMA((2 * WEIGHT_PARTS + rows // PROJECT_ROWS,)),
            pltpu.SemaphoreType.DMA((2 * (rows // PROJECT_ROWS),)),
        ],
        cost_estimate=pl.CostEstimate(
            flops=4 * rows * model * columns,
            bytes_accessed=2 * (rows * model + 2 * model * columns + 2 * rows * columns),
            transcendentals=0,
        ),
        name="project",
    )(prefix, w_key, w_value)


def attend(keep_blocks, keep_count, latent_pos, queries, both):
    ctx_count, head_count, latent_rows, head_width = queries.shape
    _, pairs, rows, _ = both.shape
    columns = pairs * PAIR
    latents = latent_pos.shape[0]
    tiles = latents // LANES
    heads_here = head_width // HD
    small = queries.dtype
    packed_rows = latent_rows * head_width // LANES + 2 * heads_here
    return pl.pallas_call(
        functools.partial(attend_kernel, chunk=ATTEND_ROWS),
        in_specs=[VMEM, VMEM, VMEM, HBM, HBM],
        out_specs=HBM,
        out_shape=jax.ShapeDtypeStruct((ctx_count, head_count, packed_rows, LANES), small),
        scratch_shapes=[
            pltpu.SMEM(keep_blocks.shape, jnp.int32),
            pltpu.VMEM((tiles, rows, LANES), jnp.float32),
            pltpu.VMEM((2, pairs, rows, PAIR), small),
            pltpu.VMEM((rows, 2 * LANES), jnp.float32),
            pltpu.VMEM((rows, 2 * LANES), jnp.float32),
            pltpu.VMEM((head_width // PAIR, 2, LANES), jnp.float32),
            pltpu.VMEM((ctx_count, head_count, packed_rows, LANES), small),
            pltpu.SemaphoreType.DMA,
            pltpu.SemaphoreType.DMA((2, pairs)),
            pltpu.SemaphoreType.DMA((tiles, head_count)),
        ],
        compiler_params=pltpu.CompilerParams(vmem_limit_bytes=ATTEND_GRANT),
        cost_estimate=pl.CostEstimate(
            flops=16 * rows * columns * latents,
            bytes_accessed=4 * rows * columns,
            transcendentals=rows * columns * latents // HD,
        ),
        name="attend",
    )(keep_count, latent_pos.reshape(1, latents), queries, keep_blocks, both)


def join_kernel(parts_ref, self_score_ref, self_value_ref, out_ref, turned_ref):
    sources = parts_ref.shape[0]
    latent_rows, width = out_ref.shape
    heads = width // HD
    per_head = width // PAIR
    data_rows = per_head * latent_rows
    wide = parts_ref[:, data_rows:, :].astype(jnp.float32)
    logs = wide + pltpu.roll(wide, heads, 1)
    top = jnp.max(logs, axis=0)
    weights = jnp.exp(logs - top[None])
    sums = jnp.sum(weights, axis=0)
    turned_ref[:, : sources * 8] = weights.reshape(sources * 8, LANES).T
    filler = jnp.zeros((LANES - 16, LANES), jnp.float32)
    turned_ref[:, sources * 8 :] = jnp.concatenate([top, sums, filler], axis=0).T
    lane = (lax.axis_index("ctx") * latent_rows) % LANES
    mine = turned_ref[pl.ds(pl.multiple_of(lane, 8), latent_rows), :]
    half = lax.broadcasted_iota(jnp.int32, (latent_rows, PAIR), 1) < HD

    def widen(first):
        left = jnp.broadcast_to(mine[:, first : first + 1], (latent_rows, PAIR))
        right = jnp.broadcast_to(mine[:, first + 1 : first + 2], (latent_rows, PAIR))
        return jnp.where(half, left, right)

    for j in range(per_head):
        columns = slice(j * PAIR, (j + 1) * PAIR)
        total = jnp.zeros((latent_rows, PAIR), jnp.float32)
        for s in range(sources):
            part = parts_ref[s, j * latent_rows : (j + 1) * latent_rows, :].astype(jnp.float32)
            total = total + widen(8 * s + 2 * j) * part
        kept_top = widen(8 * sources + 2 * j)
        kept_sum = widen(8 * sources + 8 + 2 * j)
        self_score = self_score_ref[:, columns]
        final_top = jnp.maximum(kept_top, self_score)
        keep = jnp.exp(kept_top - final_top)
        self_weight = jnp.exp(self_score - final_top)
        denominator = kept_sum * keep + self_weight
        numerator = total * keep + self_weight * self_value_ref[:, columns].astype(jnp.float32)
        out_ref[:, columns] = (numerator / denominator).astype(jnp.bfloat16)


def per_device(prefix, keep_blocks, keep_count, latent_inputs, latent_pos, w_query, w_key, w_value):
    head_count = lax.axis_size("head")
    ctx_count = lax.axis_size("ctx")
    device_count = head_count * ctx_count
    head_width = w_query.shape[1]
    model = prefix.shape[1]
    latent_rows = latent_inputs.shape[0]
    axes = ("ctx", "head")
    small = jnp.bfloat16

    copies = pl.pallas_call(
        query_kernel,
        in_specs=[HBM] * 2,
        out_specs=HBM,
        out_shape=jax.ShapeDtypeStruct((device_count, latent_rows, head_width), small),
        scratch_shapes=[
            pltpu.VMEM(latent_inputs.shape, small),
            pltpu.VMEM(w_query.shape, small),
            pltpu.VMEM((latent_rows, head_width), small),
            pltpu.SemaphoreType.DMA((2,)),
            pltpu.SemaphoreType.DMA((device_count,)),
        ],
        name="query",
    )(latent_inputs, w_query)
    queries = lax.all_to_all(copies, axes, split_axis=0, concat_axis=0, tiled=True)
    queries = queries.reshape(ctx_count, head_count, latent_rows, head_width)

    both = project(prefix, w_key, w_value)
    packed = attend(keep_blocks, keep_count, latent_pos, queries, both)
    packed_rows = packed.shape[2]
    arrived = lax.all_to_all(
        packed.reshape(device_count, packed_rows, LANES), axes, split_axis=0, concat_axis=0, tiled=True
    )

    self_score, self_value = pl.pallas_call(
        self_kernel,
        in_specs=[HBM, VMEM, HBM, HBM, HBM],
        out_specs=[VMEM] * 2,
        out_shape=[
            jax.ShapeDtypeStruct((latent_rows, head_width), jnp.float32),
            jax.ShapeDtypeStruct((latent_rows, head_width), small),
        ],
        scratch_shapes=[
            pltpu.VMEM((latent_rows, head_width), small),
            pltpu.VMEM((model, head_width), small),
            pltpu.VMEM((model, head_width), small),
            pltpu.SemaphoreType.DMA((3,)),
        ],
        compiler_params=pltpu.CompilerParams(vmem_limit_bytes=VMEM_GRANT),
        cost_estimate=pl.CostEstimate(
            flops=4 * latent_rows * model * head_width,
            bytes_accessed=4 * model * head_width,
            transcendentals=0,
        ),
        name="own",
    )(packed, latent_inputs, copies, w_key, w_value)

    return pl.pallas_call(
        join_kernel,
        in_specs=[VMEM] * 3,
        out_specs=VMEM,
        out_shape=jax.ShapeDtypeStruct((latent_rows, head_width), small),
        scratch_shapes=[pltpu.VMEM((LANES, device_count * 8 + LANES), jnp.float32)],
        compiler_params=pltpu.CompilerParams(vmem_limit_bytes=VMEM_GRANT),
        name="join",
    )(arrived, self_score, self_value)


def solution(mesh):
    return jax.shard_map(
        per_device,
        mesh=mesh,
        in_specs=(
            P(("ctx", "head"), None),
            P("head", "ctx", None),
            P("head", "ctx"),
            P("ctx", None),
            P(),
            P(None, "head"),
            P(),
            P(),
        ),
        out_specs=P("ctx", "head"),
        check_vma=False,
    )
```

```python
import functools

import jax
import jax.numpy as jnp
from jax import lax
from jax.experimental import pallas as pl
from jax.experimental.pallas import tpu as pltpu
from jax.sharding import PartitionSpec as P

HD = 64
BLOCK = 128
PAIR = 2 * HD
LANES = 128

PROJECT_ROWS = 512
AHEAD = 2
WEIGHT_PARTS = 2
ATTEND_ROWS = 256
ATTEND_GRANT = 50 * 2**20
VMEM_GRANT = 12 * 2**20

NEG_FILL = -1e30
EPSILON = 1e-06

FAR = 2**30

NT = (((1,), (1,)), ((), ()))


def normalize(source_rows):
    wide_rows = source_rows.astype(jnp.float32)
    factor = lax.rsqrt(jnp.mean(wide_rows * wide_rows, axis=-1, keepdims=True) + EPSILON)
    return (wide_rows * factor).astype(jnp.bfloat16)

VMEM = pl.BlockSpec(memory_space=pltpu.VMEM)
SMEM = pl.BlockSpec(memory_space=pltpu.SMEM)
HBM = pl.BlockSpec(memory_space=pltpu.HBM)


def query_kernel(latent_hbm, w_query_hbm, out_hbm, latent_ref, w_query_ref, query_ref, in_sem, out_sem):
    latent_copy = pltpu.make_async_copy(latent_hbm, latent_ref, in_sem.at[0])
    weight_copy = pltpu.make_async_copy(w_query_hbm, w_query_ref, in_sem.at[1])
    weight_copy.start()
    latent_copy.start()
    latent_copy.wait()
    normed = normalize(latent_ref[...])
    weight_copy.wait()
    query = jnp.dot(normed, w_query_ref[...], preferred_element_type=jnp.float32) * HD ** (-0.5)
    query = query.astype(jnp.bfloat16)
    for k in range(out_hbm.shape[0]):
        query_ref[k] = query
    out_copy = pltpu.make_async_copy(query_ref, out_hbm, out_sem)
    out_copy.start()
    out_copy.wait()


def self_kernel(
    after_hbm, latent_ref, query_hbm, w_key_hbm, w_value_hbm, score_ref, value_ref, query_ref, key_ref, column_ref, sem
):
    latent_rows, width = query_ref.shape
    mine = pl.ds(pl.multiple_of(lax.axis_index("head") * width, width), width)
    query_copy = pltpu.make_async_copy(query_hbm.at[0], query_ref, sem.at[0])
    key_copy = pltpu.make_async_copy(w_key_hbm.at[:, mine], key_ref, sem.at[1])
    value_copy = pltpu.make_async_copy(w_value_hbm.at[:, mine], column_ref, sem.at[2])
    query_copy.start()
    key_copy.start()
    value_copy.start()
    normed = normalize(latent_ref[...])
    key_copy.wait()
    key = jnp.dot(normed, key_ref[...], preferred_element_type=jnp.float32).astype(jnp.bfloat16)
    query_copy.wait()
    products = query_ref[...].astype(jnp.float32) * key.astype(jnp.float32)
    for first in range(0, width, HD):
        score = jnp.sum(products[:, first : first + HD], axis=1, keepdims=True)
        score_ref[:, first : first + HD] = jnp.broadcast_to(score, (latent_rows, HD))
    value_copy.wait()
    value = jnp.dot(normed, column_ref[...], preferred_element_type=jnp.float32)
    value_ref[...] = value.astype(jnp.bfloat16)


def project_kernel(
    prefix_hbm, w_key_hbm, w_value_hbm, both_hbm, prefix_ref, w_key_ref, w_value_ref, both_ref, in_sem, out_sem, *, tile
):
    rows = prefix_ref.shape[0]
    pairs = both_ref.shape[1]
    row_copies = [
        pltpu.make_async_copy(
            prefix_hbm.at[pl.ds(r, tile)], prefix_ref.at[pl.ds(r, tile)], in_sem.at[r // tile]
        )
        for r in range(0, rows, tile)
    ]
    columns = w_key_ref.shape[1]
    width = columns // WEIGHT_PARTS

    def part_copies(hbm, ref, first):
        return [
            pltpu.make_async_copy(
                hbm.at[:, pl.ds(k * width, width)], ref.at[:, pl.ds(k * width, width)], in_sem.at[first + k]
            )
            for k in range(WEIGHT_PARTS)
        ]

    first = rows // tile
    key_copies = part_copies(w_key_hbm, w_key_ref, first)
    value_copies = part_copies(w_value_hbm, w_value_ref, first + WEIGHT_PARTS)
    row_copies[0].start()
    for copy in key_copies + value_copies + row_copies[1:]:
        copy.start()
    out_copies = []

    def normed_rows(r):
        row_copies[r // tile].wait()
        return normalize(prefix_ref[r : r + tile, :])

    def multiply(normed, ref, copies, k, r):
        if r == 0:
            copies[k].wait()
        part = jnp.dot(
            normed, ref[:, k * width : (k + 1) * width], preferred_element_type=jnp.float32
        )
        return part.astype(jnp.bfloat16)

    def leave(which, r):
        span = pl.ds(r, tile)
        copy = pltpu.make_async_copy(
            both_ref.at[which, :, span, :],
            both_hbm.at[which, :, span, :],
            out_sem.at[2 * (r // tile) + which],
        )
        copy.start()
        out_copies.append(copy)

    def turn(part, k, r):
        for p in range(width // PAIR):
            for b in range(0, tile, BLOCK):
                both_ref[1, k * (width // PAIR) + p, r + b : r + b + BLOCK, :] = part[
                    b : b + BLOCK, p * PAIR : (p + 1) * PAIR
                ].T

    waiting = None
    normed = normed_rows(0)
    for r in range(0, rows, tile):
        for k in range(WEIGHT_PARTS):
            part = multiply(normed, w_key_ref, key_copies, k, r)
            for p in range(width // PAIR):
                both_ref[0, k * (width // PAIR) + p, r : r + tile, :] = part[:, p * PAIR : (p + 1) * PAIR]
            if waiting is not None:
                turn(*waiting)
                leave(1, waiting[2])
                waiting = None
        leave(0, r)
        following = None
        for k in range(WEIGHT_PARTS):
            part = multiply(normed, w_value_ref, value_copies, k, r)
            if k == 0 and r + tile < rows:
                following = normed_rows(r + tile)
            if waiting is not None:
                turn(*waiting)
            waiting = (part, k, r)
        normed = following
    turn(*waiting)
    leave(1, waiting[2])
    for copy in out_copies:
        copy.wait()


def attend_kernel(
    count_ref, pos_ref, query_ref, list_hbm, both_hbm, out_hbm,
    list_ref, bias_ref, both_ref, even_ref, odd_ref, log_ref, out_ref, list_sem, sem, out_sem, *, chunk
):
    _, pairs, rows, _ = both_ref.shape
    tiles = bias_ref.shape[0]
    blocks = rows // BLOCK

    def fetch(pair):
        return (
            pltpu.make_async_copy(both_hbm.at[0, pair], both_ref.at[0, pair], sem.at[0, pair]),
            pltpu.make_async_copy(both_hbm.at[1, pair], both_ref.at[1, pair], sem.at[1, pair]),
        )

    list_copy = pltpu.make_async_copy(list_hbm, list_ref, list_sem)
    list_copy.start()
    for p in range(min(AHEAD, pairs)):
        for copy in fetch(p):
            copy.start()
    shard = lax.axis_index("ctx") * lax.axis_size("head") + lax.axis_index("head")
    count = jnp.broadcast_to(count_ref[...], (BLOCK, LANES))
    row_iota = lax.broadcasted_iota(jnp.int32, (BLOCK, LANES), 0)
    list_copy.wait()
    for j in range(blocks):
        block = list_ref[0, 0, j]
        span = pl.ds(pl.multiple_of(block * BLOCK, BLOCK), BLOCK)
        start = (shard * blocks + block) * BLOCK
        for t in range(tiles):
            pos = pos_ref[:, t * LANES : (t + 1) * LANES]
            allowed = jnp.logical_and(row_iota < pos - start, count > j)
            bias_ref[t, span, :] = jnp.where(allowed, 0.0, NEG_FILL)
    ctx_count, head_count, latent_rows, head_width = query_ref.shape
    ctx_tile = LANES // latent_rows
    per_head = head_width // PAIR
    heads_here = head_width // HD
    steps = tiles * pairs
    half = lax.broadcasted_iota(jnp.int32, (LANES, PAIR), 1) < HD

    data_rows = per_head * latent_rows

    def send(tile, group):
        span = pl.ds(tile * ctx_tile, ctx_tile)
        return pltpu.make_async_copy(
            out_ref.at[span, group], out_hbm.at[span, group], out_sem.at[tile, group]
        )

    def place(step):
        tile, pair = step // pairs, step % pairs
        return tile, pair, pair // per_head, pair % per_head

    def spread_of(step):
        tile, _, group, j = place(step)
        query = query_ref[
            pl.ds(tile * ctx_tile, ctx_tile), group, :, pl.ds(pl.multiple_of(j * PAIR, PAIR), PAIR)
        ].reshape(LANES, PAIR)
        zero = jnp.zeros_like(query)
        return jnp.concatenate([jnp.where(half, query, zero), jnp.where(half, zero, query)], axis=0)

    def score_part(step, spread, r, store_ref, top8):
        tile, pair, _, _ = place(step)
        scores = lax.dot_general(
            both_ref[0, pair, r : r + chunk, :], spread, NT, preferred_element_type=jnp.float32
        )
        bias = bias_ref[tile, r : r + chunk, :]
        scores = scores + jnp.concatenate([bias, bias], axis=1)
        store_ref[r : r + chunk, :] = scores
        return jnp.maximum(top8, jnp.max(scores.reshape(chunk // 8, 8, 2 * LANES), axis=0))

    def weigh_part(step, r, load_ref, top, sum8, total):
        pair = place(step)[1]
        weights = jnp.exp(load_ref[r : r + chunk, :] - top)
        sum8 = sum8 + jnp.sum(weights.reshape(chunk // 8, 8, 2 * LANES), axis=0)
        values = [both_ref[1, pair, b : b + BLOCK, :] for b in range(r, r + chunk, BLOCK)]
        total = total + jnp.dot(
            jnp.concatenate(values, axis=1),
            weights.astype(jnp.bfloat16),
            preferred_element_type=jnp.float32,
        )
        return sum8, total

    def finish(step, top, sum8, total):
        tile, pair, group, j = place(step)
        sums = jnp.sum(sum8, axis=0, keepdims=True)
        factor = 1.0 / sums
        own = jnp.concatenate(
            [total[:HD, :LANES] * factor[:, :LANES], total[HD:, LANES:] * factor[:, LANES:]], axis=0
        )
        out_ref[
            pl.ds(tile * ctx_tile, ctx_tile),
            group,
            pl.ds(pl.multiple_of(j * latent_rows, latent_rows), latent_rows),
            :,
        ] = own.T.astype(jnp.bfloat16).reshape(ctx_tile, latent_rows, PAIR)
        log_sum = top + jnp.log(sums)
        log_ref[j] = jnp.concatenate([log_sum[:, :LANES], log_sum[:, LANES:]], axis=0)

    def depart(step):
        tile, _, group, j = place(step)

        @pl.when(j == per_head - 1)
        def _():
            logs = jnp.concatenate([log_ref[k] for k in range(per_head)], axis=0)
            high = logs.astype(jnp.bfloat16)
            low = logs - high.astype(jnp.float32)
            pieces = jnp.concatenate([high.astype(jnp.float32), low], axis=0).astype(jnp.bfloat16)
            for c in range(ctx_tile):
                out_ref[tile * ctx_tile + c, group, data_rows : data_rows + 2 * heads_here, :] = pieces
            send(tile, group).start()

    lowest = jnp.full((8, 2 * LANES), NEG_FILL, jnp.float32)
    none = jnp.zeros((8, 2 * LANES), jnp.float32)
    empty = jnp.zeros((PAIR, 2 * LANES), jnp.float32)
    chunks = range(0, rows, chunk)

    def arrive(step):
        @pl.when(step < pairs)
        def _():
            for copy in fetch(step):
                copy.wait()

        @pl.when(step + AHEAD < pairs)
        def _():
            for copy in fetch(step + AHEAD):
                copy.start()

    def both(step, store_ref, load_ref, top):
        arrive(step)
        spread = spread_of(step)
        top8, sum8, total = lowest, none, empty
        for r in chunks:
            top8 = score_part(step, spread, r, store_ref, top8)
            sum8, total = weigh_part(step - 1, r, load_ref, top, sum8, total)
        finish(step - 1, top, sum8, total)
        depart(step - 1)
        return jnp.max(top8, axis=0, keepdims=True)

    arrive(0)
    spread = spread_of(0)
    top8 = lowest
    for r in chunks:
        top8 = score_part(0, spread, r, even_ref, top8)
    top = jnp.max(top8, axis=0, keepdims=True)

    def turn(k, top):
        top = both(2 * k + 1, odd_ref, even_ref, top)
        return both(2 * k + 2, even_ref, odd_ref, top)

    top = lax.fori_loop(0, steps // 2 - 1, turn, top)
    top = both(steps - 1, odd_ref, even_ref, top)
    sum8, total = none, empty
    for r in chunks:
        sum8, total = weigh_part(steps - 1, r, odd_ref, top, sum8, total)
    finish(steps - 1, top, sum8, total)
    depart(steps - 1)

    for tile in range(tiles):
        for group in range(head_count):
            send(tile, group).wait()


def project(prefix, w_key, w_value):
    rows, model = prefix.shape
    columns = w_key.shape[1]
    pairs = columns // PAIR
    small = prefix.dtype
    return pl.pallas_call(
        functools.partial(project_kernel, tile=PROJECT_ROWS),
        in_specs=[HBM] * 3,
        out_specs=HBM,
        out_shape=jax.ShapeDtypeStruct((2, pairs, rows, PAIR), small),
        scratch_shapes=[
            pltpu.VMEM(prefix.shape, small),
            pltpu.VMEM(w_key.shape, small),
            pltpu.VMEM(w_value.shape, small),
            pltpu.VMEM((2, pairs, rows, PAIR), small),
            pltpu.SemaphoreType.DMA((2 * WEIGHT_PARTS + rows // PROJECT_ROWS,)),
            pltpu.SemaphoreType.DMA((2 * (rows // PROJECT_ROWS),)),
        ],
        cost_estimate=pl.CostEstimate(
            flops=4 * rows * model * columns,
            bytes_accessed=2 * (rows * model + 2 * model * columns + 2 * rows * columns),
            transcendentals=0,
        ),
        name="project",
    )(prefix, w_key, w_value)


def attend(keep_blocks, keep_count, latent_pos, queries, both):
    ctx_count, head_count, latent_rows, head_width = queries.shape
    _, pairs, rows, _ = both.shape
    columns = pairs * PAIR
    latents = latent_pos.shape[0]
    tiles = latents // LANES
    heads_here = head_width // HD
    small = queries.dtype
    packed_rows = latent_rows * head_width // LANES + 2 * heads_here
    return pl.pallas_call(
        functools.partial(attend_kernel, chunk=ATTEND_ROWS),
        in_specs=[VMEM, VMEM, VMEM, HBM, HBM],
        out_specs=HBM,
        out_shape=jax.ShapeDtypeStruct((ctx_count, head_count, packed_rows, LANES), small),
        scratch_shapes=[
            pltpu.SMEM(keep_blocks.shape, jnp.int32),
            pltpu.VMEM((tiles, rows, LANES), jnp.float32),
            pltpu.VMEM((2, pairs, rows, PAIR), small),
            pltpu.VMEM((rows, 2 * LANES), jnp.float32),
            pltpu.VMEM((rows, 2 * LANES), jnp.float32),
            pltpu.VMEM((head_width // PAIR, 2, LANES), jnp.float32),
            pltpu.VMEM((ctx_count, head_count, packed_rows, LANES), small),
            pltpu.SemaphoreType.DMA,
            pltpu.SemaphoreType.DMA((2, pairs)),
            pltpu.SemaphoreType.DMA((tiles, head_count)),
        ],
        compiler_params=pltpu.CompilerParams(vmem_limit_bytes=ATTEND_GRANT),
        cost_estimate=pl.CostEstimate(
            flops=16 * rows * columns * latents,
            bytes_accessed=4 * rows * columns,
            transcendentals=rows * columns * latents // HD,
        ),
        name="attend",
    )(keep_count, latent_pos.reshape(1, latents), queries, keep_blocks, both)


def join_kernel(parts_ref, self_score_ref, self_value_ref, out_ref, turned_ref):
    sources = parts_ref.shape[0]
    latent_rows, width = out_ref.shape
    heads = width // HD
    per_head = width // PAIR
    data_rows = per_head * latent_rows
    wide = parts_ref[:, data_rows:, :].astype(jnp.float32)
    logs = wide + pltpu.roll(wide, heads, 1)
    top = jnp.max(logs, axis=0)
    weights = jnp.exp(logs - top[None])
    sums = jnp.sum(weights, axis=0)
    turned_ref[:, : sources * 8] = weights.reshape(sources * 8, LANES).T
    filler = jnp.zeros((LANES - 16, LANES), jnp.float32)
    turned_ref[:, sources * 8 :] = jnp.concatenate([top, sums, filler], axis=0).T
    lane = (lax.axis_index("ctx") * latent_rows) % LANES
    mine = turned_ref[pl.ds(pl.multiple_of(lane, 8), latent_rows), :]
    half = lax.broadcasted_iota(jnp.int32, (latent_rows, PAIR), 1) < HD

    def widen(first):
        left = jnp.broadcast_to(mine[:, first : first + 1], (latent_rows, PAIR))
        right = jnp.broadcast_to(mine[:, first + 1 : first + 2], (latent_rows, PAIR))
        return jnp.where(half, left, right)

    for j in range(per_head):
        columns = slice(j * PAIR, (j + 1) * PAIR)
        total = jnp.zeros((latent_rows, PAIR), jnp.float32)
        for s in range(sources):
            part = parts_ref[s, j * latent_rows : (j + 1) * latent_rows, :].astype(jnp.float32)
            total = total + widen(8 * s + 2 * j) * part
        kept_top = widen(8 * sources + 2 * j)
        kept_sum = widen(8 * sources + 8 + 2 * j)
        self_score = self_score_ref[:, columns]
        final_top = jnp.maximum(kept_top, self_score)
        keep = jnp.exp(kept_top - final_top)
        self_weight = jnp.exp(self_score - final_top)
        denominator = kept_sum * keep + self_weight
        numerator = total * keep + self_weight * self_value_ref[:, columns].astype(jnp.float32)
        out_ref[:, columns] = (numerator / denominator).astype(jnp.bfloat16)


def per_device(prefix, keep_blocks, keep_count, latent_inputs, latent_pos, w_query, w_key, w_value):
    head_count = lax.axis_size("head")
    ctx_count = lax.axis_size("ctx")
    device_count = head_count * ctx_count
    head_width = w_query.shape[1]
    model = prefix.shape[1]
    latent_rows = latent_inputs.shape[0]
    axes = ("ctx", "head")
    small = jnp.bfloat16

    copies = pl.pallas_call(
        query_kernel,
        in_specs=[HBM] * 2,
        out_specs=HBM,
        out_shape=jax.ShapeDtypeStruct((device_count, latent_rows, head_width), small),
        scratch_shapes=[
            pltpu.VMEM(latent_inputs.shape, small),
            pltpu.VMEM(w_query.shape, small),
            pltpu.VMEM((device_count, latent_rows, head_width), small),
            pltpu.SemaphoreType.DMA((2,)),
            pltpu.SemaphoreType.DMA,
        ],
        name="query",
    )(latent_inputs, w_query)
    queries = lax.all_to_all(copies, axes, split_axis=0, concat_axis=0, tiled=True)
    queries = queries.reshape(ctx_count, head_count, latent_rows, head_width)

    both = project(prefix, w_key, w_value)
    packed = attend(keep_blocks, keep_count, latent_pos, queries, both)
    packed_rows = packed.shape[2]
    arrived = lax.all_to_all(
        packed.reshape(device_count, packed_rows, LANES), axes, split_axis=0, concat_axis=0, tiled=True
    )

    self_score, self_value = pl.pallas_call(
        self_kernel,
        in_specs=[HBM, VMEM, HBM, HBM, HBM],
        out_specs=[VMEM] * 2,
        out_shape=[
            jax.ShapeDtypeStruct((latent_rows, head_width), jnp.float32),
            jax.ShapeDtypeStruct((latent_rows, head_width), small),
        ],
        scratch_shapes=[
            pltpu.VMEM((latent_rows, head_width), small),
            pltpu.VMEM((model, head_width), small),
            pltpu.VMEM((model, head_width), small),
            pltpu.SemaphoreType.DMA((3,)),
        ],
        compiler_params=pltpu.CompilerParams(vmem_limit_bytes=VMEM_GRANT),
        cost_estimate=pl.CostEstimate(
            flops=4 * latent_rows * model * head_width,
            bytes_accessed=4 * model * head_width,
            transcendentals=0,
        ),
        name="own",
    )(packed, latent_inputs, copies, w_key, w_value)

    return pl.pallas_call(
        join_kernel,
        in_specs=[VMEM] * 3,
        out_specs=VMEM,
        out_shape=jax.ShapeDtypeStruct((latent_rows, head_width), small),
        scratch_shapes=[pltpu.VMEM((LANES, device_count * 8 + LANES), jnp.float32)],
        compiler_params=pltpu.CompilerParams(vmem_limit_bytes=VMEM_GRANT),
        name="join",
    )(arrived, self_score, self_value)


def solution(mesh):
    return jax.shard_map(
        per_device,
        mesh=mesh,
        in_specs=(
            P(("ctx", "head"), None),
            P("head", "ctx", None),
            P("head", "ctx"),
            P("ctx", None),
            P(),
            P(None, "head"),
            P(),
            P(),
        ),
        out_specs=P("ctx", "head"),
        check_vma=False,
    )
```
